1024 devices in a mesh: layer: 32 (over z_lo, x), shard: 32 (over y, z_hi, core).
Axes of the slice: x: 4, y: 8, z: 16 (z_hi: 2, z_lo: 8; z = z_hi * 8 + z_lo), core: 2. Of those that a mesh axis runs over, the one named last changes fastest.
Arguments:
- gate_grad: bfloat16 [256, 2048, 512], P('layer', 'shard'), parts along dimension 0, may hold values from -400 to 400
- gate_moment: bfloat16 [256, 2048, 512], P('layer', 'shard'), parts along dimension 0, may hold values from -120 to 120
- down_grad: bfloat16 [256, 2048, 512], P('layer', 'shard'), parts along dimension 0, may hold values from -400 to 400
- down_moment: bfloat16 [256, 2048, 512], P('layer', 'shard'), parts along dimension 0, may hold values from -120 to 120
Outputs:
- gate_update: bfloat16 [256, 2048, 512], P('layer', 'shard'), parts along dimension 0
- down_update: bfloat16 [256, 2048, 512], P('layer', 'shard'), parts along dimension 0
The draws below stay inside these ranges and needn't reach their ends.
There are 32 independent parts, one for each index of `layer`. The reference program is written for one: setup_inputs(seed, part) draws one part's arguments, and reference() takes and returns one part's arrays. A program takes and returns all parts, laid end to end along the dimension named above; each array names one. Nothing has to cross between parts.
All inputs are finite; a program needn't handle non-finite values.
Results may differ from the reference program's by a relative error of at most 0.0068.
Values may be sent and summed in bfloat16 or wider, within the bound.
No kernel may reach another device: no remote copies, remote signals or barrier semaphores. Data moves between devices by JAX's collectives and lax.ppermute only.
A program may use at most 32 MiB of HBM per device.

```python
import math
import jax
import jax.numpy as jnp
from jax import lax

D = 2048
FF = 512
ITERS = 2
EXPERTS = 8
N_SHARD = 32


def scaled_field(key):
    keys = jax.random.split(key, 3)
    row_scale = jnp.exp(jax.random.uniform(keys[0], (EXPERTS, D, 1), jnp.float32, 0.0, math.log(10.0)))
    column_scale = jnp.exp(jax.random.uniform(keys[1], (EXPERTS, 1, FF), jnp.float32, 0.0, math.log(10.0)))
    entries = jax.random.truncated_normal(keys[2], -4.0, 4.0, (EXPERTS, D, FF), jnp.float32)
    return (entries * row_scale * column_scale).astype(jnp.bfloat16)


def draw_gate_grad(key, part):
    return scaled_field(jax.random.fold_in(key, 11))


def draw_down_grad(key, part):
    return scaled_field(jax.random.fold_in(key, 23))


def block_scale(key, shape, cuts, least, high):
    level, own = 1.0, jax.random.fold_in(key, 6)
    for axis_at, parts in cuts:
        heights = jnp.exp(jax.random.uniform(jax.random.fold_in(own, axis_at), (parts,), jnp.float32, least / len(cuts), high / len(cuts)))
        level = level * jnp.repeat(heights, shape[axis_at] // parts).reshape([-1 if axis == axis_at else 1 for axis in range(len(shape))])
    return level


def scatter_about(stream_key, shape, spread, limit, pieces=(), kind=jnp.bfloat16):
    gain = block_scale(stream_key, shape, pieces, -0.22, 0.18) if pieces else 1.0
    values = jax.random.normal(stream_key, shape, jnp.float32) * spread * gain
    return jnp.minimum(jnp.maximum(values, -limit), limit).astype(kind)


def setup_inputs(seed: int = 0, part: int = 0) -> dict:
    splits = jax.random.split(jax.random.key(seed), 5)
    own_keys = jax.random.split(jax.random.fold_in(splits[4], part), 5)
    gate_grad = draw_gate_grad(jax.random.fold_in(jax.random.fold_in(splits[4], part), 71), part)
    gate_moment = scatter_about(own_keys[1], (EXPERTS, D, FF), 20.0, 120.0, ((1, 32),))
    down_grad = draw_down_grad(jax.random.fold_in(jax.random.fold_in(splits[4], part), 71), part)
    down_moment = scatter_about(own_keys[3], (EXPERTS, D, FF), 20.0, 120.0, ((1, 32),))
    return dict(gate_grad=gate_grad, gate_moment=gate_moment, down_grad=down_grad, down_moment=down_moment)


MOMENTUM_RATE = 0.95
COEF_A = 3.4445
COEF_B = -4.775
COEF_C = 2.0315
EPSILON = 1e-07

def blended(gradient, moment):
    buffer = MOMENTUM_RATE * moment.astype(jnp.float32) + gradient.astype(jnp.float32)
    return (gradient.astype(jnp.float32) + MOMENTUM_RATE * buffer).astype(jnp.bfloat16)

def transposed_product(first_matrix, second_matrix):
    return lax.dot_general(first_matrix.astype(jnp.float32), second_matrix.astype(jnp.float32), (((0,), (0,)), ((), ())), preferred_element_type=jnp.float32)

def quintic(current):
    square = jnp.dot(current, current, preferred_element_type=jnp.float32)
    identity = jnp.eye(current.shape[0], dtype=jnp.float32)
    return (COEF_A * identity + COEF_B * current.astype(jnp.float32) + COEF_C * square).astype(jnp.bfloat16)

def orthogonal_update(matrix):
    blocks = matrix.reshape(N_SHARD, 4, D // (4 * N_SHARD), FF)
    total = jnp.zeros((FF, FF), jnp.float32)
    for member in range(4):
        quarter = blocks[:, member].reshape(-1, FF)
        partial_value = lax.optimization_barrier(transposed_product(quarter, quarter).astype(jnp.bfloat16))
        total = total + partial_value.astype(jnp.float32)
    factor = 1.0 / (jnp.sqrt(jnp.trace(total)) + EPSILON)
    scaled = (total * (factor * factor)).astype(jnp.bfloat16)
    combined = quintic(scaled)
    for iteration in range(ITERS - 1):
        product = jnp.dot(scaled, combined, preferred_element_type=jnp.float32).astype(jnp.bfloat16)
        current = transposed_product(combined, product).astype(jnp.bfloat16)
        combined = jnp.dot(combined, quintic(current), preferred_element_type=jnp.float32).astype(jnp.bfloat16)
    result = jnp.dot(matrix, combined, preferred_element_type=jnp.float32) * (math.sqrt(D) * factor)
    return result.astype(jnp.bfloat16)

def reference(gate_grad, gate_moment, down_grad, down_moment):
    gate_input = blended(gate_grad, gate_moment)
    down_input = blended(down_grad, down_moment)
    gate_update = lax.map(orthogonal_update, gate_input)
    down_update = lax.map(orthogonal_update, down_input)
    return (gate_update, down_update)
```

```python
import math

import jax
import jax.numpy as jnp
from jax import lax
from jax.sharding import Mesh
from jax.sharding import PartitionSpec as P

D = 2048
SHARD = ("y", "z_hi", "core")
HALF = ("y", "core")

MOMENTUM_RATE = 0.95
COEF_A = 3.4445
COEF_B = -4.775
COEF_C = 2.0315
EPSILON = 1e-07


def blended(gradient, moment):
    buffer = MOMENTUM_RATE * moment.astype(jnp.float32) + gradient.astype(jnp.float32)
    return (gradient.astype(jnp.float32) + MOMENTUM_RATE * buffer).astype(jnp.bfloat16)


def transposed_product(first_matrix, second_matrix):
    return lax.dot_general(
        first_matrix, second_matrix, (((0,), (0,)), ((), ())), preferred_element_type=jnp.float32
    )


def quintic(current):
    square = jnp.dot(current, current, preferred_element_type=jnp.float32)
    identity = jnp.eye(current.shape[0], dtype=jnp.float32)
    return (COEF_A * identity + COEF_B * current.astype(jnp.float32) + COEF_C * square).astype(
        jnp.bfloat16
    )


def positions(size):
    shape = (size, size)
    return lax.broadcasted_iota(jnp.int32, shape, 0), lax.broadcasted_iota(jnp.int32, shape, 1)


def pack(gram):
    half = gram.shape[0] // 2
    row, column = positions(half)
    first, second = gram[:half, :half], gram[half:, half:]
    diagonal = jnp.sum(jnp.where(row == column, first, 0.0), 0)
    return jnp.concatenate(
        (
            gram[:half, half:],
            jnp.where(row < column, first, second),
            jnp.broadcast_to(diagonal, (8, half)),
        ),
        0,
    )


def unpack(packed):
    half = packed.shape[1]
    row, column = positions(half)
    corner, both, diagonal = packed[:half], packed[half : 2 * half], packed[2 * half]
    mirrored = both.T
    first = jnp.where(row < column, both, jnp.where(row == column, diagonal, mirrored))
    second = jnp.where(row < column, mirrored, both)
    total = jnp.concatenate(
        (jnp.concatenate((first, corner), 1), jnp.concatenate((corner.T, second), 1)), 0
    )
    trace = jnp.sum(diagonal) + jnp.sum(jnp.where(row == column, both, 0.0))
    return total, trace


def polish(owned_rows, packed_total):
    total, trace = unpack(packed_total)
    factor = 1.0 / (jnp.sqrt(trace) + EPSILON)
    scaled = (total * (factor * factor)).astype(jnp.bfloat16)
    combined = quintic(scaled)
    product = jnp.dot(scaled, combined, preferred_element_type=jnp.float32).astype(jnp.bfloat16)
    current = transposed_product(combined, product).astype(jnp.bfloat16)
    combined = jnp.dot(combined, quintic(current), preferred_element_type=jnp.float32).astype(
        jnp.bfloat16
    )
    result = jnp.dot(owned_rows, combined, preferred_element_type=jnp.float32) * (
        math.sqrt(D) * factor
    )
    return result.astype(jnp.bfloat16)


def exchange(blocks):
    return lax.all_to_all(blocks, HALF, split_axis=0, concat_axis=0, tiled=True)


def shards(gate_grad, gate_moment, down_grad, down_moment):
    experts, row_count, columns = gate_grad.shape
    stacked = jnp.concatenate(
        (blended(gate_grad, gate_moment), blended(down_grad, down_moment)), 0
    )
    owned_rows = exchange(stacked).reshape(-1, columns)
    own = pack(transposed_product(owned_rows, owned_rows)).astype(jnp.bfloat16)
    own = lax.optimization_barrier(own)
    far = lax.ppermute(own, "z_hi", [(0, 1), (1, 0)])
    result = polish(owned_rows, own.astype(jnp.float32) + far.astype(jnp.float32))
    restored = exchange(result.reshape(2 * experts, row_count, columns))
    return restored[:experts], restored[experts:]


def solution(mesh):
    split = Mesh(
        mesh.devices.reshape(mesh.shape["layer"], -1, 2, 2), ("layer", "y", "z_hi", "core")
    )
    spec = P("layer", SHARD, None)
    return jax.shard_map(
        shards, mesh=split, in_specs=(spec,) * 4, out_specs=(spec, spec), check_vma=False
    )
```

```python
import math

import jax
import jax.numpy as jnp
from jax import lax
from jax.experimental import pallas as pl
from jax.experimental.pallas import tpu as pltpu
from jax.sharding import Mesh
from jax.sharding import PartitionSpec as P

D = 2048
SHARD = ("y", "z_hi", "core")
HALF = ("y", "core")
GRANT = 16 << 20

MOMENTUM_RATE = 0.95
COEF_A = 3.4445
COEF_B = -4.775
COEF_C = 2.0315
EPSILON = 1e-07

IN_VMEM = pl.BlockSpec(memory_space=pltpu.VMEM)


def blended(gradient, moment):
    buffer = MOMENTUM_RATE * moment.astype(jnp.float32) + gradient.astype(jnp.float32)
    return (gradient.astype(jnp.float32) + MOMENTUM_RATE * buffer).astype(jnp.bfloat16)


def blend_all(gate_grad, gate_moment, down_grad, down_moment):
    return blended(
        jnp.concatenate((gate_grad, down_grad), 0), jnp.concatenate((gate_moment, down_moment), 0)
    )


def positions(size):
    shape = (size, size)
    return lax.broadcasted_iota(jnp.int32, shape, 0), lax.broadcasted_iota(jnp.int32, shape, 1)


def transposed_product(first_matrix, second_matrix):
    return lax.dot_general(
        first_matrix, second_matrix, (((0,), (0,)), ((), ())), preferred_element_type=jnp.float32
    )


def gram_kernel(rows, packed):
    half = rows.shape[1] // 2
    row, column = positions(half)
    packed[:half] = transposed_product(rows[:, :half], rows[:, half:]).astype(jnp.bfloat16)
    first = transposed_product(rows[:, :half], rows[:, :half])
    second = transposed_product(rows[:, half:], rows[:, half:])
    packed[half : 2 * half] = jnp.where(row < column, first, second).astype(jnp.bfloat16)
    diagonal = jnp.sum(jnp.where(row == column, first, 0.0), 0, keepdims=True)
    packed[2 * half :] = jnp.broadcast_to(diagonal, (8, half)).astype(jnp.bfloat16)


def gram(rows):
    half = rows.shape[1] // 2
    return pl.pallas_call(
        gram_kernel,
        out_shape=jax.ShapeDtypeStruct((2 * half + 8, half), jnp.bfloat16),
        in_specs=[IN_VMEM],
        out_specs=IN_VMEM,
        compiler_params=pltpu.CompilerParams(vmem_limit_bytes=GRANT),
        name="gram",
    )(rows)


def product(left, right):
    return jnp.dot(left, right, preferred_element_type=jnp.float32)


def quintic(current):
    row, column = positions(current.shape[0])
    linear = COEF_B * current.astype(jnp.float32) + jnp.where(row == column, COEF_A, 0.0)
    return (linear + COEF_C * product(current, current)).astype(jnp.bfloat16)


def polish_kernel(rows, own, far, out, scaled):
    half = own.shape[1]
    row, column = positions(half)
    packed = own[...].astype(jnp.float32) + far[...].astype(jnp.float32)
    corner, both, diagonal = packed[:half], packed[half : 2 * half], packed[2 * half : 2 * half + 1]
    mirrored = both.T
    first = jnp.where(row < column, both, jnp.where(row == column, diagonal, mirrored))
    second = jnp.where(row < column, mirrored, both)
    on_diagonal = jnp.where(row == column, both, 0.0)
    trace = jnp.sum(
        diagonal + jnp.sum(on_diagonal, 0, keepdims=True), 1, keepdims=True
    )
    factor = 1.0 / (jnp.sqrt(trace) + EPSILON)
    square = factor * factor
    scaled[:half, :half] = (first * square).astype(jnp.bfloat16)
    scaled[half:, half:] = (second * square).astype(jnp.bfloat16)
    corner = corner * square
    scaled[:half, half:] = corner.astype(jnp.bfloat16)
    scaled[half:, :half] = corner.T.astype(jnp.bfloat16)
    current = scaled[...]
    combined = quintic(current)
    current = product(combined, product(current, combined).astype(jnp.bfloat16))
    combined = product(combined, quintic(current.astype(jnp.bfloat16))).astype(jnp.bfloat16)
    out[...] = (product(rows[...], combined) * (math.sqrt(D) * factor)).astype(jnp.bfloat16)


def polish(rows, own, far):
    columns = rows.shape[1]
    return pl.pallas_call(
        polish_kernel,
        out_shape=jax.ShapeDtypeStruct(rows.shape, jnp.bfloat16),
        in_specs=[IN_VMEM] * 3,
        out_specs=IN_VMEM,
        scratch_shapes=[pltpu.VMEM((columns, columns), jnp.bfloat16)],
        compiler_params=pltpu.CompilerParams(vmem_limit_bytes=GRANT),
        name="polish",
    )(rows, own, far)


def exchange(blocks):
    return lax.all_to_all(blocks, HALF, split_axis=0, concat_axis=0, tiled=True)


def shards(gate_grad, gate_moment, down_grad, down_moment):
    experts, row_count, columns = gate_grad.shape
    stacked = blend_all(gate_grad, gate_moment, down_grad, down_moment)
    owned_rows = exchange(stacked).reshape(-1, columns)
    own = gram(owned_rows)
    far = lax.ppermute(own, "z_hi", [(0, 1), (1, 0)])
    result = polish(owned_rows, own, far)
    restored = exchange(result.reshape(2 * experts, row_count, columns))
    return restored[:experts], restored[experts:]


def solution(mesh):
    split = Mesh(
        mesh.devices.reshape(mesh.shape["layer"], -1, 2, 2), ("layer", "y", "z_hi", "core")
    )
    spec = P("layer", SHARD, None)
    return jax.shard_map(
        shards, mesh=split, in_specs=(spec,) * 4, out_specs=(spec, spec), check_vma=False
    )
```

```python
import math

import jax
import jax.numpy as jnp
from jax import lax
from jax.experimental import pallas as pl
from jax.experimental.pallas import tpu as pltpu
from jax.sharding import Mesh
from jax.sharding import PartitionSpec as P

D = 2048
SHARD = ("y", "z_hi", "core")
HALF = ("y", "core")
GRANT = 16 << 20

MOMENTUM_RATE = 0.95
COEF_A = 3.4445
COEF_B = -4.775
COEF_C = 2.0315
EPSILON = 1e-07

IN_VMEM = pl.BlockSpec(memory_space=pltpu.VMEM)


def blended(gradient, moment):
    buffer = MOMENTUM_RATE * moment.astype(jnp.float32) + gradient.astype(jnp.float32)
    return (gradient.astype(jnp.float32) + MOMENTUM_RATE * buffer).astype(jnp.bfloat16)


def blend_all(gate_grad, gate_moment, down_grad, down_moment):
    return blended(
        jnp.concatenate((gate_grad, down_grad), 0), jnp.concatenate((gate_moment, down_moment), 0)
    )


def positions(size):
    shape = (size, size)
    return lax.broadcasted_iota(jnp.int32, shape, 0), lax.broadcasted_iota(jnp.int32, shape, 1)


def transposed_product(first_matrix, second_matrix):
    return lax.dot_general(
        first_matrix, second_matrix, (((0,), (0,)), ((), ())), preferred_element_type=jnp.float32
    )


def gram_kernel(rows, packed):
    half = rows.shape[1] // 2
    row, column = positions(half)
    packed[:half] = transposed_product(rows[:, :half], rows[:, half:]).astype(jnp.bfloat16)
    first = transposed_product(rows[:, :half], rows[:, :half])
    second = transposed_product(rows[:, half:], rows[:, half:])
    packed[half : 2 * half] = jnp.where(row < column, first, second).astype(jnp.bfloat16)
    diagonal = jnp.sum(jnp.where(row == column, first, 0.0), 0, keepdims=True)
    packed[2 * half :] = jnp.broadcast_to(diagonal, (8, half)).astype(jnp.bfloat16)


def gram(rows):
    half = rows.shape[1] // 2
    return pl.pallas_call(
        gram_kernel,
        out_shape=jax.ShapeDtypeStruct((2 * half + 8, half), jnp.bfloat16),
        in_specs=[IN_VMEM],
        out_specs=IN_VMEM,
        compiler_params=pltpu.CompilerParams(vmem_limit_bytes=GRANT),
        name="gram",
    )(rows)


def product(left, right):
    return jnp.dot(left, right, preferred_element_type=jnp.float32)


def quintic(current):
    row, column = positions(current.shape[0])
    linear = COEF_B * current.astype(jnp.float32) + jnp.where(row == column, COEF_A, 0.0)
    return (linear + COEF_C * product(current, current)).astype(jnp.bfloat16)


def polish_kernel(rows, halves, out, scaled):
    half = halves.shape[2]
    row, column = positions(half)
    packed = halves[0].astype(jnp.float32) + halves[1].astype(jnp.float32)
    corner, both, diagonal = packed[:half], packed[half : 2 * half], packed[2 * half : 2 * half + 1]
    mirrored = both.T
    first = jnp.where(row < column, both, jnp.where(row == column, diagonal, mirrored))
    second = jnp.where(row < column, mirrored, both)
    on_diagonal = jnp.where(row == column, both, 0.0)
    trace = jnp.sum(
        diagonal + jnp.sum(on_diagonal, 0, keepdims=True), 1, keepdims=True
    )
    factor = 1.0 / (jnp.sqrt(trace) + EPSILON)
    square = factor * factor
    scaled[:half, :half] = (first * square).astype(jnp.bfloat16)
    scaled[half:, half:] = (second * square).astype(jnp.bfloat16)
    corner = corner * square
    scaled[:half, half:] = corner.astype(jnp.bfloat16)
    scaled[half:, :half] = corner.T.astype(jnp.bfloat16)
    current = scaled[...]
    combined = quintic(current)
    current = product(combined, product(current, combined).astype(jnp.bfloat16))
    combined = product(combined, quintic(current.astype(jnp.bfloat16))).astype(jnp.bfloat16)
    out[...] = (product(rows[...], combined) * (math.sqrt(D) * factor)).astype(jnp.bfloat16)


def polish(rows, halves):
    columns = rows.shape[1]
    return pl.pallas_call(
        polish_kernel,
        out_shape=jax.ShapeDtypeStruct(rows.shape, jnp.bfloat16),
        in_specs=[IN_VMEM] * 2,
        out_specs=IN_VMEM,
        scratch_shapes=[pltpu.VMEM((columns, columns), jnp.bfloat16)],
        compiler_params=pltpu.CompilerParams(vmem_limit_bytes=GRANT),
        name="polish",
    )(rows, halves)


def exchange(blocks):
    return lax.all_to_all(blocks, HALF, split_axis=0, concat_axis=0, tiled=True)


def shards(gate_grad, gate_moment, down_grad, down_moment):
    experts, row_count, columns = gate_grad.shape
    stacked = blend_all(gate_grad, gate_moment, down_grad, down_moment)
    owned_rows = exchange(stacked).reshape(-1, columns)
    own = gram(owned_rows)
    result = polish(owned_rows, lax.all_gather(own, "z_hi"))
    restored = exchange(result.reshape(2 * experts, row_count, columns))
    return restored[:experts], restored[experts:]


def solution(mesh):
    split = Mesh(
        mesh.devices.reshape(mesh.shape["layer"], -1, 2, 2), ("layer", "y", "z_hi", "core")
    )
    spec = P("layer", SHARD, None)
    return jax.shard_map(
        shards, mesh=split, in_specs=(spec,) * 4, out_specs=(spec, spec), check_vma=False
    )
```
